32 devices in a mesh: grp: 2 (over y), depth: 4 (over x, core), shot: 4 (over z).
Axes of the slice: x: 2, y: 2, z: 4, core: 2. Of those that a mesh axis runs over, the one named last changes fastest.
Arguments:
- forward: bfloat16 [4, 8, 32, 32, 128], P(None, ('grp', 'shot'), 'depth'), parts along dimension 1, may hold values from -6 to 6
- adjoint_last: float32 [8, 32, 32, 128], P(('grp', 'shot'), 'depth'), parts along dimension 0, may hold values from -6 to 6
- adjoint_late: float32 [8, 32, 32, 128], P(('grp', 'shot'), 'depth'), parts along dimension 0, may hold values from -6 to 6
- residuals: float32 [8, 4, 256], P(('grp', 'shot')), parts along dimension 0, may hold values from -6 to 6
- source_cells: int32 [8, 3], P('grp'), parts along dimension 0, may hold values from 0 to 127, as said below
- receiver_cells: int32 [8, 256, 3], P('grp'), parts along dimension 0, may hold values from 0 to 127, as said below
- assignment: int32 [8], P('grp'), parts along dimension 0, may hold values from 0 to 3, each once
- model: float32 [6, 32, 16, 64], P(None, ('grp', 'depth'), 'shot'), parts along dimension 1, may hold values from -0.4 to 2, as said below
Outputs:
- adjoint_first: float32 [8, 32, 32, 128], P(('grp', 'shot'), 'depth'), parts along dimension 0
- gradients: float32 [6, 32, 16, 64], P(None, ('grp', 'depth'), 'shot'), parts along dimension 1
The draws below stay inside these ranges and needn't reach their ends.
There are 2 independent parts, one for each index of `grp`. The reference program is written for one: setup_inputs(seed, part) draws one part's arguments, and reference() takes and returns one part's arrays. A program takes and returns all parts, laid end to end along the dimension named above; each array names one. Nothing has to cross between parts.
Inputs may be any that keep to these rules, and one draw needn't show every extreme that they name: `source_cells`: each row holds the depth, second and third cell index of a source inside the grid of 32 x 32 x 128 cells. `receiver_cells`: each entry holds the depth, second and third cell index of a receiver inside the grid; receivers may share a cell. `assignment`: each survey row is used by exactly one shot. `model`: channel 0 (depth with depth) lies in 1 to 2; channels 1 and 2 (second with second, third with third) lie in 0.25 to 1; channels 3 to 5 (depth with second, depth with third, second with third) lie in -0.4 to 0.4.
All inputs are finite; a program needn't handle non-finite values.
Results may differ from the reference program's by a relative error of at most 0.0003.
Values sent between devices are 32-bit elements; how exact they have to be, the bound alone decides.
A program may use at most 128 MiB of HBM per device.

```python
import math
import jax
import jax.numpy as jnp
from jax import lax

NX = 32
NY = 128
STEPS = 4
NREC = 256
MUTE = 3
NZ = 32
ZC = 16
XC = 16
YC = 64
SHOTS = 4


def draw_model(key, part):
    depth_key, side_key, second_key = jax.random.split(jax.random.fold_in(key, 17), 3)
    single = (1, ZC, XC, YC)
    double = (2, ZC, XC, YC)
    triple = (3, ZC, XC, YC)
    vertical = jnp.exp(jax.random.uniform(depth_key, single, jnp.float32, 0.0, math.log(2.0)))
    lateral = jnp.exp(jax.random.uniform(side_key, double, jnp.float32, math.log(0.25), 0.0))
    crossed = jax.random.uniform(second_key, triple, jnp.float32, -0.3, 0.3)
    return jnp.concatenate([vertical, lateral, crossed], axis=0)


def cell_columns(key, leading):
    depth_key, row_key, column_key = jax.random.split(key, 3)
    return jnp.stack([jax.random.randint(depth_key, leading, 0, NZ, dtype=jnp.int32), jax.random.randint(row_key, leading, 0, NX, dtype=jnp.int32), jax.random.randint(column_key, leading, 0, NY, dtype=jnp.int32)], axis=-1)


def draw_source_cells(key, part):
    return cell_columns(jax.random.fold_in(key, 23), (SHOTS,))


def draw_receiver_cells(key, part):
    return cell_columns(jax.random.fold_in(key, 29), (SHOTS, NREC))


def levels(stream_key, extent, pieces, least, top_value):
    loudness = 1.0
    for dim, shards_of in pieces:
        heights = jax.random.uniform(jax.random.fold_in(jax.random.fold_in(stream_key, 6), dim), (shards_of,), jnp.float32, least / len(pieces), top_value / len(pieces))
        loudness = loudness * jnp.repeat(jnp.exp(heights), extent[dim] // shards_of).reshape((-1,) + (1,) * (len(extent) - 1 - dim))
    return loudness


def centred(stream_key, shape, width, limit, cuts=(), kind=jnp.bfloat16):
    entries = jax.random.normal(stream_key, shape, jnp.float32) * width
    if len(cuts) > 0:
        entries = levels(stream_key, shape, cuts, -0.22, 0.18) * entries
    return jnp.clip(entries, min=-limit, max=limit).astype(kind)


def setup_inputs(seed: int = 0, part: int = 0) -> dict:
    streams_of = jax.random.split(jax.random.key(seed), 9)
    part_keys = jax.random.split(jax.random.fold_in(streams_of[8], part), 9)
    forward = centred(part_keys[0], (STEPS, SHOTS, NZ, NX, NY), 1.0, 6.0, ((1, 4), (2, 4)))
    adjoint_last = centred(part_keys[1], (SHOTS, NZ, NX, NY), 1.0, 6.0, ((0, 4), (1, 4)), jnp.float32)
    adjoint_late = centred(part_keys[2], (SHOTS, NZ, NX, NY), 1.0, 6.0, ((0, 4), (1, 4)), jnp.float32)
    residuals = centred(part_keys[3], (SHOTS, STEPS, NREC), 1.0, 6.0, ((0, 4),), jnp.float32)
    source_cells = draw_source_cells(jax.random.fold_in(jax.random.fold_in(streams_of[8], part), 71), part)
    receiver_cells = draw_receiver_cells(jax.random.fold_in(jax.random.fold_in(streams_of[8], part), 71), part)
    assignment = jax.random.permutation(part_keys[6], SHOTS).astype(jnp.int32)
    model = draw_model(jax.random.fold_in(jax.random.fold_in(streams_of[8], part), 71), part)
    return {"forward": forward, "adjoint_last": adjoint_last, "adjoint_late": adjoint_late, "residuals": residuals, "source_cells": source_cells, "receiver_cells": receiver_cells, "assignment": assignment, "model": model}


TIME_SQUARED = 0.2


def refine(coarse, dimension):
    coarse_count = coarse.shape[dimension]
    later_rows = lax.slice_in_dim(coarse, 1, coarse_count, axis=dimension)
    edge_row = lax.slice_in_dim(coarse, coarse_count - 1, coarse_count, axis=dimension)
    middle = (coarse + jnp.concatenate([later_rows, edge_row], axis=dimension)) * 0.5
    merged = jnp.stack([coarse, middle], axis=dimension + 1)
    new_shape = coarse.shape[:dimension] + (2 * coarse_count,) + coarse.shape[dimension + 1:]
    return merged.reshape(new_shape)


def coarsen(fine_cells, dimension):
    half_count = fine_cells.shape[dimension] // 2
    paired = fine_cells.reshape(fine_cells.shape[:dimension] + (half_count, 2) + fine_cells.shape[dimension + 1:])
    even_cells = lax.index_in_dim(paired, 0, dimension + 1, keepdims=False)
    odd_cells = lax.index_in_dim(paired, 1, dimension + 1, keepdims=False)
    first_odd = lax.slice_in_dim(odd_cells, 0, 1, axis=dimension)
    earlier = jnp.concatenate([jnp.zeros_like(first_odd), lax.slice_in_dim(odd_cells, 0, half_count - 1, axis=dimension)], axis=dimension)
    tail_part = jnp.concatenate([jnp.zeros_like(lax.slice_in_dim(odd_cells, 1, half_count, axis=dimension)), lax.slice_in_dim(odd_cells, half_count - 1, half_count, axis=dimension)], axis=dimension)
    return even_cells + 0.5 * odd_cells + 0.5 * earlier + 0.5 * tail_part


def window(padded, offsets):
    depth_step, row_step, column_step = offsets
    inner_depth = padded.shape[-3] - 2
    inner_rows = padded.shape[-2] - 2
    inner_columns = padded.shape[-1] - 2
    return padded[..., 1 + depth_step:1 + depth_step + inner_depth, 1 + row_step:1 + row_step + inner_rows, 1 + column_step:1 + column_step + inner_columns]


def derivatives(padded):
    centre = window(padded, (0, 0, 0))

    def second(offsets, opposite):
        return window(padded, offsets) - 2.0 * centre + window(padded, opposite)

    def cross(upper_one, upper_two, lower_one, lower_two):
        return (window(padded, upper_one) - window(padded, upper_two) - window(padded, lower_one) + window(padded, lower_two)) * 0.25

    return jnp.stack([
        second((1, 0, 0), (-1, 0, 0)),
        second((0, 1, 0), (0, -1, 0)),
        second((0, 0, 1), (0, 0, -1)),
        cross((1, 1, 0), (1, -1, 0), (-1, 1, 0), (-1, -1, 0)),
        cross((1, 0, 1), (1, 0, -1), (-1, 0, 1), (-1, 0, -1)),
        cross((0, 1, 1), (0, 1, -1), (0, -1, 1), (0, -1, -1)),
    ], axis=0)


def reference(forward, adjoint_last, adjoint_late, residuals, source_cells, receiver_cells, assignment, model):
    coefficients = refine(refine(refine(model, 1), 3), 2)
    depth_cells = jnp.arange(NZ, dtype=jnp.int32)
    row_cells = jnp.arange(NX, dtype=jnp.int32)
    column_cells = jnp.arange(NY, dtype=jnp.int32)

    def one_shot(summed, shot_index):
        geometry = assignment[shot_index]
        sources = source_cells[geometry]
        receivers = receiver_cells[geometry]
        flat_index = ((receivers[:, 0] * NX + receivers[:, 1]) * NY + receivers[:, 2]).astype(jnp.int32)
        current = adjoint_last[shot_index]
        previous = adjoint_late[shot_index]
        totals = jnp.zeros((6, NZ, NX, NY), jnp.float32)
        for step_index in range(STEPS):
            slopes = derivatives(jnp.pad(current, 1))
            totals = totals + forward[step_index, shot_index].astype(jnp.float32)[None] * slopes
            updated = 2.0 * current - previous + TIME_SQUARED * jnp.sum(coefficients * slopes, axis=0)
            updated = updated.reshape(-1).at[flat_index].add(residuals[shot_index, step_index]).reshape(current.shape)
            previous, current = current, updated
        muted = ((jnp.abs(depth_cells - sources[0]) <= MUTE)[:, None, None]
                 & (jnp.abs(row_cells - sources[1]) <= MUTE)[None, :, None]
                 & (jnp.abs(column_cells - sources[2]) <= MUTE)[None, None, :])
        kept = jnp.where(muted[None], jnp.zeros_like(totals), totals)
        summed = summed + coarsen(coarsen(coarsen(kept, 3), 2), 1)
        return summed, current

    start = jnp.zeros((6, ZC, XC, YC), jnp.float32)
    summed, finals = lax.scan(one_shot, start, jnp.arange(SHOTS, dtype=jnp.int32))
    return finals, summed / STEPS
```

```python
import functools

import jax
import jax.numpy as jnp
from jax import lax
from jax.experimental import pallas as pl
from jax.experimental.pallas import tpu as pltpu
from jax.sharding import PartitionSpec as P

MUTE = 3
TIME_SQUARED = 0.2
MESH = pl.DeviceIdType.MESH
F32 = jnp.float32
BF16 = jnp.bfloat16


def split_dot(exact, values, contract):
    high = values.astype(BF16)
    low = (values - high.astype(F32)).astype(BF16)
    return exact_dot(exact, high, contract) + exact_dot(exact, low, contract)


def exact_dot(exact, part, contract):
    if contract == "values_left":
        return lax.dot_general(part, exact, (((1,), (0,)), ((), ())), preferred_element_type=F32)
    return lax.dot_general(exact, part, (((1,), (1,)), ((), ())), preferred_element_type=F32)


def kernel(
    forward, last, late, residuals, receivers, model, assignment, sources,
    adjoint_first, gradients,
    gbuf, coarse_y, fine_x, coef, field_a, field_b, inj, totals, restr, lhs_main, lhs_rim,
    send_main, send_rim, recv_main, recv_rim, total,
    gs_sem, gr_sem, hs_sem, hr_sem, fs_sem, fr_sem, ms_sem, mr_sem, rs_sem, rr_sem,
):
    steps = forward.shape[0]
    depth_len, rows, cols = last.shape[1:]
    coarse_len, rl, half_cols = model.shape[1:]
    shots = lax.axis_size("shot")
    depths = lax.axis_size("depth")
    me = lax.axis_index("shot")
    d = lax.axis_index("depth")
    has_up = d > 0
    has_down = d < depths - 1
    halo = steps
    reach = steps - 1
    window = depth_len + 2 * reach
    coarse_rows = shots * rl

    barrier = pltpu.get_barrier_semaphore()

    def greet(device):
        pl.semaphore_signal(barrier, inc=1, device_id=device, device_id_type=MESH)

    for o in range(1, shots):
        greet({"shot": lax.rem(me + o, shots)})

    @pl.when(has_up)
    def _():
        for o in range(shots):
            greet({"depth": d - 1, "shot": lax.rem(me + o, shots)})

    @pl.when(has_down)
    def _():
        for o in range(shots):
            greet({"depth": d + 1, "shot": lax.rem(me + o, shots)})

    for l in range(coarse_len):
        for c in range(3):
            pair = jnp.concatenate([model[c, l], model[c + 3, l]], axis=-1)
            first = ((l % 2) * 3 + c) * rl
            gbuf[me, 1 + l // 2, first:first + rl, :] = pair

    beside = jnp.where(has_up, shots, 0) + jnp.where(has_down, shots, 0)
    pl.semaphore_wait(barrier, shots - 1 + beside)

    def gather_copy(o, sending):
        peer = lax.rem(me + o, shots) if sending else lax.rem(me + shots - o, shots)
        slot = me if sending else peer
        return pltpu.make_async_remote_copy(
            src_ref=gbuf.at[slot, 1:3], dst_ref=gbuf.at[slot, 1:3],
            send_sem=gs_sem.at[o], recv_sem=gr_sem.at[slot],
            device_id={"shot": peer}, device_id_type=MESH)

    for o in range(1, shots):
        gather_copy(o, True).start()

    def field_down(which, source, dest, width, sending):
        return pltpu.make_async_remote_copy(
            src_ref=source.at[0, depth_len - width:depth_len],
            dst_ref=dest.at[halo - width:halo],
            send_sem=hs_sem.at[0, which], recv_sem=hr_sem.at[0, which],
            device_id={"depth": d + 1 if sending else d - 1}, device_id_type=MESH)

    def field_up(which, source, dest, width, sending):
        return pltpu.make_async_remote_copy(
            src_ref=source.at[0, 0:width],
            dst_ref=dest.at[halo + depth_len:halo + depth_len + width],
            send_sem=hs_sem.at[1, which], recv_sem=hr_sem.at[1, which],
            device_id={"depth": d - 1 if sending else d + 1}, device_id_type=MESH)

    both = ((0, last, field_a, halo), (1, late, field_b, reach))

    def model_down(slot, sending):
        return pltpu.make_async_remote_copy(
            src_ref=gbuf.at[slot, 2], dst_ref=gbuf.at[slot, 0],
            send_sem=fs_sem.at[0, slot], recv_sem=fr_sem.at[0, slot],
            device_id={"depth": d + 1 if sending else d - 1}, device_id_type=MESH)

    def model_up(slot, sending):
        return pltpu.make_async_remote_copy(
            src_ref=gbuf.at[slot, 1], dst_ref=gbuf.at[slot, 3],
            send_sem=fs_sem.at[1, slot], recv_sem=fr_sem.at[1, slot],
            device_id={"depth": d - 1 if sending else d + 1}, device_id_type=MESH)

    def spread(slot):
        @pl.when(has_down)
        def _():
            model_down(slot, True).start()

        @pl.when(has_up)
        def _():
            model_up(slot, True).start()

    spread(me)

    @pl.when(has_down)
    def _():
        for args in both:
            field_down(*args, True).start()

    @pl.when(has_up)
    def _():
        for args in both:
            field_up(*args, True).start()

    zeros_halo = jnp.zeros((halo, rows, cols), F32)

    @pl.when(jnp.logical_not(has_up))
    def _():
        field_a[0:halo] = zeros_halo
        field_b[0:halo] = zeros_halo

    @pl.when(jnp.logical_not(has_down))
    def _():
        field_a[halo + depth_len:] = zeros_halo
        field_b[halo + depth_len:] = zeros_halo

    field_a[halo:halo + depth_len] = last[0]
    field_b[halo:halo + depth_len] = late[0]

    shot = assignment[me]
    picked = []
    for k in range(3):
        chosen = jnp.zeros((1, receivers.shape[2]), jnp.int32)
        for j in range(receivers.shape[1]):
            chosen = chosen + jnp.where(shot == j, receivers[k, j:j + 1, :], 0)
        picked.append(chosen)
    place = (picked[0] - d * depth_len + reach) * rows + picked[1]
    count = receivers.shape[2]
    spot = lax.broadcasted_iota(jnp.int32, (window * rows, count), 0) == place
    spot = jnp.where(spot, 1.0, 0.0).astype(BF16)
    column = lax.broadcasted_iota(jnp.int32, (cols, count), 0) == picked[2]
    for i in range(steps):
        placed = jnp.where(column, residuals[0, i:i + 1, :], 0.0)
        inj[i] = split_dot(spot, placed, "values_right").reshape(window, rows, cols)

    for o in range(1, shots):
        gather_copy(o, False).wait_recv()
        spread(lax.rem(me + shots - o, shots))

    refine_y = jnp.zeros((2 * half_cols, 2 * cols), F32)
    c_in = lax.broadcasted_iota(jnp.int32, (2 * half_cols, 2 * cols), 0)
    f_out = lax.broadcasted_iota(jnp.int32, (2 * half_cols, 2 * cols), 1)
    same = (c_in >= half_cols) == (f_out >= cols)
    ci = jnp.where(c_in >= half_cols, c_in - half_cols, c_in)
    fo = jnp.where(f_out >= cols, f_out - cols, f_out)
    weight = jnp.where(fo == 2 * ci, 1.0, 0.0)
    weight = weight + jnp.where((fo == 2 * ci + 1) | (fo == 2 * ci - 1), 0.5, 0.0)
    weight = weight + jnp.where((fo == cols - 1) & (ci == half_cols - 1), 0.5, 0.0)
    refine_y = jnp.where(same, weight, 0.0).astype(BF16)

    @pl.when(has_up)
    def _():
        for slot in range(shots):
            model_down(slot, False).wait_recv()

    @pl.when(has_down)
    def _():
        for slot in range(shots):
            model_up(slot, False).wait_recv()

    pairs = 6 * rl
    for group in range(4):
        for s in range(shots):
            refined = split_dot(refine_y, gbuf[s, group], "values_left") * TIME_SQUARED
            for l2 in range(2):
                for c in range(3):
                    first = (l2 * 3 + c) * rl
                    piece = refined[first:first + rl]
                    coarse_y[c, 2 * group + l2, s * rl:(s + 1) * rl, :] = piece[:, 0:cols]
                    coarse_y[c + 3, 2 * group + l2, s * rl:(s + 1) * rl, :] = piece[:, cols:]

    row16 = lax.broadcasted_iota(jnp.int32, (coarse_rows, cols), 0)
    for c in range(6):
        scale = 1.0 if c < 3 else 0.25
        for l in range(2 * 4):
            here = coarse_y[c, l] * scale
            after = jnp.where(row16 == coarse_rows - 1, here, pltpu.roll(here, coarse_rows - 1, 0))
            fine_x[c, l, pl.ds(0, coarse_rows, stride=2), :] = here
            fine_x[c, l, pl.ds(1, coarse_rows, stride=2), :] = (here + after) * 0.5
    for c in range(6):
        for f in range(-reach, depth_len + reach):
            k = f // 2 + 2
            value = fine_x[c, k]
            if f % 2:
                after = fine_x[c, k + 1]
                if f == depth_len - 1:
                    after = jnp.where(has_down, after, value)
                value = (value + after) * 0.5
            if f < 0:
                value = jnp.where(has_up, value, 0.0)
            if f >= depth_len:
                value = jnp.where(has_down, value, 0.0)
            coef[c, f + reach] = value

    @pl.when(has_up)
    def _():
        for args in both:
            field_down(*args, False).wait_recv()

    @pl.when(has_down)
    def _():
        for args in both:
            field_up(*args, False).wait_recv()

    lane = lax.broadcasted_iota(jnp.int32, (rows, cols), 1)
    row = lax.broadcasted_iota(jnp.int32, (rows, cols), 0)
    lane_first, lane_last = lane == 0, lane == cols - 1
    row_first, row_last = row == 0, row == rows - 1

    def right(v):
        return jnp.where(lane_last, 0.0, pltpu.roll(v, cols - 1, 1))

    def left(v):
        return jnp.where(lane_first, 0.0, pltpu.roll(v, 1, 1))

    def under(v):
        return jnp.where(row_last, 0.0, pltpu.roll(v, rows - 1, 0))

    def over(v):
        return jnp.where(row_first, 0.0, pltpu.roll(v, 1, 0))

    def sides(v):
        xp, xm, yp, ym = under(v), over(v), right(v), left(v)
        return v, xp - xm, yp - ym, xp + xm, yp + ym

    source_z = sources[shot, 0] - d * depth_len
    source_x = sources[shot, 1]
    source_y = sources[shot, 2]
    mute_xy = (jnp.abs(row - source_x) <= MUTE) & (jnp.abs(lane - source_y) <= MUTE)

    current, previous = field_a, field_b
    for i in range(steps):
        extra = reach - i
        final = i == steps - 1

        def layer(f, before, here, after, owned, i=i, final=final, cur=current, prev=previous):
            v, dx, dy, sx, sy = here
            twice = 2.0 * v
            slopes = (
                after[0] - twice + before[0],
                sx - twice,
                sy - twice,
                after[1] - before[1],
                after[2] - before[2],
                under(dy) - over(dy),
            )
            acc = coef[0, f + reach] * slopes[0]
            for c in range(1, 6):
                acc = acc + coef[c, f + reach] * slopes[c]
            new = twice - prev[f + halo] + acc + inj[i, f + reach]
            if final:
                adjoint_first[0, f] = new
            else:
                prev[f + halo] = new
            if owned:
                wave = forward[i, 0, f].astype(F32)
                cross_wave = wave * 0.25
                for c in range(6):
                    term = (wave if c < 3 else cross_wave) * slopes[c]
                    if i:
                        term = totals[c, f] + term
                    if final:
                        hidden = mute_xy & (jnp.abs(f - source_z) <= MUTE)
                        term = jnp.where(hidden, 0.0, term)
                    totals[c, f] = term

        def run(first, stop, owned, carry, cur=current, layer=layer):
            def body(f, carry):
                before, here = carry
                after = sides(cur[f + 1 + halo])
                layer(f, before, here, after, owned)
                return here[:3], after
            return lax.fori_loop(first, stop, body, carry)

        carry = (sides(current[halo - extra - 1])[:3], sides(current[halo - extra]))
        if extra:
            carry = run(-extra, 0, False, carry)
        carry = run(0, depth_len, True, carry)
        if extra:
            carry = run(depth_len, depth_len + extra, False, carry)
        current, previous = previous, current

    fine_16 = lax.broadcasted_iota(jnp.int32, (coarse_rows, cols), 0)
    last_depth = jnp.where(has_down, 0.0, 0.5)
    for c in range(6):
        lanes = slice((c // 3) * cols, (c // 3) * cols + cols)
        for l in range(coarse_len + 1):
            if l == coarse_len:
                value = 0.5 * totals[c, depth_len - 1]
            else:
                value = totals[c, 2 * l] + 0.5 * totals[c, 2 * l + 1]
                if l:
                    value = value + 0.5 * totals[c, 2 * l - 1]
                if l == coarse_len - 1:
                    value = value + last_depth * totals[c, depth_len - 1]
            restr[c, l] = value
            even = restr[c, l, pl.ds(0, coarse_rows, stride=2), :]
            odd = restr[c, l, pl.ds(1, coarse_rows, stride=2), :]
            earlier = jnp.where(fine_16 == 0, 0.0, pltpu.roll(odd, 1, 0))
            tail = jnp.where(fine_16 == coarse_rows - 1, odd, 0.0)
            value = even + 0.5 * (odd + earlier + tail)
            for s in range(shots):
                piece = value[s * rl:(s + 1) * rl]
                if l == coarse_len:
                    lhs_rim[s, (c % 3) * rl:(c % 3 + 1) * rl, lanes] = piece
                else:
                    first = (l * 3 + c % 3) * rl
                    lhs_main[s, first:first + rl, lanes] = piece

    f_in = lax.broadcasted_iota(jnp.int32, (2 * cols, 2 * half_cols), 0)
    c_out = lax.broadcasted_iota(jnp.int32, (2 * cols, 2 * half_cols), 1)
    same = (f_in >= cols) == (c_out >= half_cols)
    fi = jnp.where(f_in >= cols, f_in - cols, f_in)
    co = jnp.where(c_out >= half_cols, c_out - half_cols, c_out)
    weight = jnp.where(fi == 2 * co, 1.0, 0.0)
    weight = weight + jnp.where((fi == 2 * co + 1) | (fi == 2 * co - 1), 0.5, 0.0)
    weight = weight + jnp.where((fi == cols - 1) & (co == half_cols - 1), 0.5, 0.0)
    coarsen_y = jnp.where(same, weight, 0.0).astype(BF16)
    main_rows, rim_rows = lhs_main.shape[1], lhs_rim.shape[1]
    outcome = split_dot(
        coarsen_y, lhs_main[...].reshape(shots * main_rows, 2 * cols), "values_left")
    send_main[...] = outcome.reshape(shots, main_rows, 2 * half_cols)
    outcome = split_dot(
        coarsen_y, lhs_rim[...].reshape(shots * rim_rows, 2 * cols), "values_left")
    send_rim[...] = outcome.reshape(shots, rim_rows, 2 * half_cols)

    def main_copy(o, sending):
        peer = lax.rem(me + o, shots) if sending else lax.rem(me + shots - o, shots)
        slot = me if sending else peer
        return pltpu.make_async_remote_copy(
            src_ref=send_main.at[peer], dst_ref=recv_main.at[slot],
            send_sem=ms_sem.at[o], recv_sem=mr_sem.at[slot],
            device_id={"shot": peer}, device_id_type=MESH)

    def rim_copy(o, sending):
        peer = lax.rem(me + o, shots) if sending else lax.rem(me + shots - o, shots)
        slot = me if sending else peer
        return pltpu.make_async_remote_copy(
            src_ref=send_rim.at[peer], dst_ref=recv_rim.at[slot],
            send_sem=rs_sem.at[o], recv_sem=rr_sem.at[slot],
            device_id={"depth": d + 1 if sending else d - 1, "shot": peer}, device_id_type=MESH)

    for o in range(1, shots):
        main_copy(o, True).start()

    @pl.when(has_down)
    def _():
        for o in range(shots):
            rim_copy(o, True).start()

    result = send_main[me]
    for o in range(1, shots):
        main_copy(o, False).wait_recv()
        result = result + recv_main[lax.rem(me + shots - o, shots)]
    total[0] = result

    @pl.when(has_up)
    def _():
        rim_sum = None
        for o in range(shots):
            rim_copy(o, False).wait_recv()
            piece = recv_rim[lax.rem(me + shots - o, shots)]
            rim_sum = piece if rim_sum is None else rim_sum + piece
        total[0, 0:3 * rl] = total[0, 0:3 * rl] + rim_sum[0:3 * rl]

    result = total[0] * (1.0 / steps)
    total[0] = result
    total[1] = pltpu.roll(result, half_cols, 1)
    for l in range(coarse_len):
        for c in range(3):
            first = (l * 3 + c) * rl
            gradients[c, l] = total[0, first:first + rl, 0:half_cols]
            gradients[c + 3, l] = total[1, first:first + rl, 0:half_cols]

    for o in range(1, shots):
        gather_copy(o, True).wait_send()
        main_copy(o, True).wait_send()

    @pl.when(has_down)
    def _():
        for args in both:
            field_down(*args, True).wait_send()
        for slot in range(shots):
            model_down(slot, True).wait_send()
        for o in range(shots):
            rim_copy(o, True).wait_send()

    @pl.when(has_up)
    def _():
        for args in both:
            field_up(*args, True).wait_send()
        for slot in range(shots):
            model_up(slot, True).wait_send()


def up8(n):
    return (n + 7) // 8 * 8


def on_device(
    forward, adjoint_last, adjoint_late, residuals, source_cells, receiver_cells, assignment, model
):
    steps, shots_here, depth_len, rows, cols = forward.shape
    channels, coarse_len, rl, half_cols = model.shape
    shots = lax.axis_size("shot")
    assert shots_here == 1 and coarse_len == 4 and steps == 4 and channels == 6
    window = depth_len + 2 * steps - 2
    coarse_rows = shots * rl
    field = (depth_len + 2 * steps, rows, cols)
    main_rows, rim_rows = up8(coarse_len * 3 * rl), up8(3 * rl)
    dma = pltpu.SemaphoreType.DMA
    vmem = pl.BlockSpec(memory_space=pltpu.VMEM)
    smem = pl.BlockSpec(memory_space=pltpu.SMEM)
    return pl.pallas_call(
        kernel,
        name="adjoint_gradient",
        out_shape=(
            jax.ShapeDtypeStruct(adjoint_last.shape, F32),
            jax.ShapeDtypeStruct(model.shape, F32),
        ),
        in_specs=[vmem] * 6 + [smem] * 2,
        out_specs=(vmem, vmem),
        scratch_shapes=[
            pltpu.VMEM((shots, 4, 6 * rl, 2 * half_cols), F32),
            pltpu.VMEM((6, 8, coarse_rows, cols), F32),
            pltpu.VMEM((6, 8, rows, cols), F32),
            pltpu.VMEM((6, window, rows, cols), F32),
            pltpu.VMEM(field, F32),
            pltpu.VMEM(field, F32),
            pltpu.VMEM((steps, window, rows, cols), F32),
            pltpu.VMEM((6, depth_len, rows, cols), F32),
            pltpu.VMEM((6, coarse_len + 1, rows, cols), F32),
            pltpu.VMEM((shots, main_rows, 2 * cols), F32),
            pltpu.VMEM((shots, rim_rows, 2 * cols), F32),
            pltpu.VMEM((shots, main_rows, 2 * half_cols), F32),
            pltpu.VMEM((shots, rim_rows, 2 * half_cols), F32),
            pltpu.VMEM((shots, main_rows, 2 * half_cols), F32),
            pltpu.VMEM((shots, rim_rows, 2 * half_cols), F32),
            pltpu.VMEM((2, main_rows, 2 * half_cols), F32),
            dma((shots,)), dma((shots,)),
            dma((2, 2)), dma((2, 2)),
            dma((2, shots)), dma((2, shots)),
            dma((shots,)), dma((shots,)),
            dma((shots,)), dma((shots,)),
        ],
        compiler_params=pltpu.CompilerParams(collective_id=0, has_side_effects=True),
    )(
        forward, adjoint_last, adjoint_late, residuals,
        jnp.transpose(receiver_cells, (2, 0, 1)), model, assignment, source_cells,
    )


def solution(mesh):
    placed = (
        P(None, ("grp", "shot"), "depth", None, None),
        P(("grp", "shot"), "depth", None, None),
        P(("grp", "shot"), "depth", None, None),
        P(("grp", "shot"), None, None),
        P("grp", None),
        P("grp", None, None),
        P("grp"),
        P(None, ("grp", "depth"), "shot", None),
    )
    return jax.shard_map(
        on_device,
        mesh=mesh,
        in_specs=placed,
        out_specs=(
            P(("grp", "shot"), "depth", None, None),
            P(None, ("grp", "depth"), "shot", None),
        ),
        check_vma=False,
    )
```

```python
import functools

import jax
import jax.numpy as jnp
from jax import lax
from jax.experimental import pallas as pl
from jax.experimental.pallas import tpu as pltpu
from jax.sharding import PartitionSpec as P

MUTE = 3
TIME_SQUARED = 0.2
MESH = pl.DeviceIdType.MESH
F32 = jnp.float32
BF16 = jnp.bfloat16


def split_dot(exact, values, contract):
    high = values.astype(BF16)
    low = (values - high.astype(F32)).astype(BF16)
    return exact_dot(exact, high, contract) + exact_dot(exact, low, contract)


def exact_dot(exact, part, contract):
    if contract == "values_left":
        return lax.dot_general(part, exact, (((1,), (0,)), ((), ())), preferred_element_type=F32)
    return lax.dot_general(exact, part, (((1,), (1,)), ((), ())), preferred_element_type=F32)


def kernel(
    forward_hbm, last_hbm, late_hbm, residuals_hbm, receivers_hbm, model_hbm, assignment, sources,
    adjoint_hbm, gradients_hbm,
    forward, last, late, residuals, receivers, model, adjoint_first, gradients,
    gbuf, coarse_y, fine_x, coef, field_a, field_b, inj, totals, restr, lhs_main, lhs_rim,
    send_main, send_rim, recv_main, recv_rim, total, coarsen_ref,
    gs_sem, gr_sem, hs_sem, hr_sem, fs_sem, fr_sem, ms_sem, mr_sem, rs_sem, rr_sem, in_sem, out_sem,
):
    steps = forward.shape[0]
    depth_len, rows, cols = last.shape[1:]
    coarse_len, rl, half_cols = model.shape[1:]
    shots = lax.axis_size("shot")
    depths = lax.axis_size("depth")
    me = lax.axis_index("shot")
    d = lax.axis_index("depth")
    has_up = d > 0
    has_down = d < depths - 1
    halo = steps
    reach = steps - 1
    window = depth_len + 2 * reach
    coarse_rows = shots * rl

    barrier = pltpu.get_barrier_semaphore()

    def greet(device):
        pl.semaphore_signal(barrier, inc=1, device_id=device, device_id_type=MESH)

    for o in range(1, shots):
        greet({"shot": lax.rem(me + o, shots)})

    @pl.when(has_up)
    def _():
        greet({"depth": d - 1})

    @pl.when(has_down)
    def _():
        greet({"depth": d + 1})

    pulls = [
        pltpu.make_async_copy(source, dest, in_sem.at[k])
        for k, (source, dest) in enumerate((
            (model_hbm, model), (last_hbm, last), (late_hbm, late), (receivers_hbm, receivers),
            (residuals_hbm, residuals), (forward_hbm, forward)))
    ]
    for pull in pulls:
        pull.start()
    pulls[0].wait()

    for l in range(coarse_len):
        for c in range(3):
            pair = jnp.concatenate([model[c, l], model[c + 3, l]], axis=-1)
            first = ((l % 2) * 3 + c) * rl
            gbuf[me, 1 + l // 2, first:first + rl, :] = pair

    beside = jnp.where(has_up, 1, 0) + jnp.where(has_down, 1, 0)
    pl.semaphore_wait(barrier, shots - 1 + beside)

    later = shots - 1 - me

    def other(t):
        return jnp.where(t < later, shots - 1 - t, t - later)

    def gather_copy(t, sending):
        peer = other(t)
        slot = me if sending else peer
        return pltpu.make_async_remote_copy(
            src_ref=gbuf.at[slot, 1:3], dst_ref=gbuf.at[slot, 1:3],
            send_sem=gs_sem.at[t], recv_sem=gr_sem.at[slot],
            device_id={"shot": peer}, device_id_type=MESH)

    for t in range(shots - 1):
        gather_copy(t, True).start()

    def field_down(which, source, dest, width, sending):
        return pltpu.make_async_remote_copy(
            src_ref=source.at[0, depth_len - width:depth_len],
            dst_ref=dest.at[halo - width:halo],
            send_sem=hs_sem.at[0, which], recv_sem=hr_sem.at[0, which],
            device_id={"depth": d + 1 if sending else d - 1}, device_id_type=MESH)

    def field_up(which, source, dest, width, sending):
        return pltpu.make_async_remote_copy(
            src_ref=source.at[0, 0:width],
            dst_ref=dest.at[halo + depth_len:halo + depth_len + width],
            send_sem=hs_sem.at[1, which], recv_sem=hr_sem.at[1, which],
            device_id={"depth": d - 1 if sending else d + 1}, device_id_type=MESH)

    both = ((0, last, field_a, halo), (1, late, field_b, reach))

    def model_down(slot, sending):
        return pltpu.make_async_remote_copy(
            src_ref=gbuf.at[slot, 2], dst_ref=gbuf.at[slot, 0],
            send_sem=fs_sem.at[0, slot], recv_sem=fr_sem.at[0, slot],
            device_id={"depth": d + 1 if sending else d - 1}, device_id_type=MESH)

    def model_up(slot, sending):
        return pltpu.make_async_remote_copy(
            src_ref=gbuf.at[slot, 1], dst_ref=gbuf.at[slot, 3],
            send_sem=fs_sem.at[1, slot], recv_sem=fr_sem.at[1, slot],
            device_id={"depth": d - 1 if sending else d + 1}, device_id_type=MESH)

    def spread(slot):
        @pl.when(has_down)
        def _():
            model_down(slot, True).start()

        @pl.when(has_up)
        def _():
            model_up(slot, True).start()

    spread(me)
    pulls[1].wait()
    pulls[2].wait()

    @pl.when(has_down)
    def _():
        for args in both:
            field_down(*args, True).start()

    @pl.when(has_up)
    def _():
        for args in both:
            field_up(*args, True).start()

    zeros_halo = jnp.zeros((halo, rows, cols), F32)

    @pl.when(jnp.logical_not(has_up))
    def _():
        field_a[0:halo] = zeros_halo
        field_b[0:halo] = zeros_halo

    @pl.when(jnp.logical_not(has_down))
    def _():
        field_a[halo + depth_len:] = zeros_halo
        field_b[halo + depth_len:] = zeros_halo

    field_a[halo:halo + depth_len] = last[0]
    field_b[halo:halo + depth_len] = late[0]

    pulls[3].wait()
    pulls[4].wait()
    shot = assignment[me]
    picked = []
    for k in range(3):
        chosen = jnp.zeros((1, receivers.shape[2]), jnp.int32)
        for j in range(receivers.shape[1]):
            chosen = chosen + jnp.where(shot == j, receivers[k, j:j + 1, :], 0)
        picked.append(chosen)
    place = (picked[0] - d * depth_len + reach) * rows + picked[1]
    count = receivers.shape[2]
    spot = lax.broadcasted_iota(jnp.int32, (window * rows, count), 0) == place
    spot = jnp.where(spot, 1.0, 0.0).astype(BF16)
    column = lax.broadcasted_iota(jnp.int32, (cols, count), 0) == picked[2]
    for i in range(steps):
        placed = jnp.where(column, residuals[0, i:i + 1, :], 0.0)
        inj[i] = split_dot(spot, placed, "values_right").reshape(window, rows, cols)

    c_in = lax.broadcasted_iota(jnp.int32, (2 * half_cols, 2 * cols), 0)
    f_out = lax.broadcasted_iota(jnp.int32, (2 * half_cols, 2 * cols), 1)
    same = (c_in >= half_cols) == (f_out >= cols)
    ci = jnp.where(c_in >= half_cols, c_in - half_cols, c_in)
    fo = jnp.where(f_out >= cols, f_out - cols, f_out)
    weight = jnp.where(fo == 2 * ci, 1.0, 0.0)
    weight = weight + jnp.where((fo == 2 * ci + 1) | (fo == 2 * ci - 1), 0.5, 0.0)
    weight = weight + jnp.where((fo == cols - 1) & (ci == half_cols - 1), 0.5, 0.0)
    refine_y = jnp.where(same, weight, 0.0).astype(BF16)

    f_in = lax.broadcasted_iota(jnp.int32, (2 * cols, 2 * half_cols), 0)
    c_out = lax.broadcasted_iota(jnp.int32, (2 * cols, 2 * half_cols), 1)
    same = (f_in >= cols) == (c_out >= half_cols)
    fi = jnp.where(f_in >= cols, f_in - cols, f_in)
    co = jnp.where(c_out >= half_cols, c_out - half_cols, c_out)
    weight = jnp.where(fi == 2 * co, 1.0, 0.0)
    weight = weight + jnp.where((fi == 2 * co + 1) | (fi == 2 * co - 1), 0.5, 0.0)
    weight = weight + jnp.where((fi == cols - 1) & (co == half_cols - 1), 0.5, 0.0)
    coarsen_y = jnp.where(same, weight, 0.0).astype(BF16)
    coarsen_ref[...] = coarsen_y

    pulls[5].wait()
    for t in range(shots - 1):
        gather_copy(t, False).wait_recv()
        spread(other(t))

    row16 = lax.broadcasted_iota(jnp.int32, (coarse_rows, cols), 0)

    def refine_group(group):
        for s in range(shots):
            refined = split_dot(refine_y, gbuf[s, group], "values_left") * TIME_SQUARED
            for l2 in range(2):
                for c in range(3):
                    first = (l2 * 3 + c) * rl
                    piece = refined[first:first + rl]
                    coarse_y[c, 2 * group + l2, s * rl:(s + 1) * rl, :] = piece[:, 0:cols]
                    coarse_y[c + 3, 2 * group + l2, s * rl:(s + 1) * rl, :] = piece[:, cols:]
        for c in range(6):
            scale = 1.0 if c < 3 else 0.25
            for l in (2 * group, 2 * group + 1):
                here = coarse_y[c, l] * scale
                after = pltpu.roll(here, coarse_rows - 1, 0)
                after = jnp.where(row16 == coarse_rows - 1, here, after)
                fine_x[c, l, pl.ds(0, coarse_rows, stride=2), :] = here
                fine_x[c, l, pl.ds(1, coarse_rows, stride=2), :] = (here + after) * 0.5

    def refine_depth(first, stop):
        for c in range(6):
            for f in range(first, stop):
                k = f // 2 + 2
                value = fine_x[c, k]
                if f % 2:
                    after = fine_x[c, k + 1]
                    if f == depth_len - 1:
                        after = jnp.where(has_down, after, value)
                    value = (value + after) * 0.5
                if f < 0:
                    value = jnp.where(has_up, value, 0.0)
                if f >= depth_len:
                    value = jnp.where(has_down, value, 0.0)
                coef[c, f + reach] = value

    refine_group(1)
    refine_group(2)
    refine_depth(0, depth_len - 1)

    @pl.when(has_up)
    def _():
        for slot in range(shots):
            model_down(slot, False).wait_recv()

    @pl.when(has_down)
    def _():
        for slot in range(shots):
            model_up(slot, False).wait_recv()

    refine_group(0)
    refine_group(3)
    refine_depth(-reach, 0)
    refine_depth(depth_len - 1, depth_len + reach)

    @pl.when(has_up)
    def _():
        for args in both:
            field_down(*args, False).wait_recv()

    @pl.when(has_down)
    def _():
        for args in both:
            field_up(*args, False).wait_recv()

    lane = lax.broadcasted_iota(jnp.int32, (rows, cols), 1)
    row = lax.broadcasted_iota(jnp.int32, (rows, cols), 0)
    lane_first, lane_last = lane == 0, lane == cols - 1
    row_first, row_last = row == 0, row == rows - 1

    def right(v):
        return jnp.where(lane_last, 0.0, pltpu.roll(v, cols - 1, 1))

    def left(v):
        return jnp.where(lane_first, 0.0, pltpu.roll(v, 1, 1))

    def under(v):
        return jnp.where(row_last, 0.0, pltpu.roll(v, rows - 1, 0))

    def over(v):
        return jnp.where(row_first, 0.0, pltpu.roll(v, 1, 0))

    def sides(v):
        xp, xm, yp, ym = under(v), over(v), right(v), left(v)
        return v, xp - xm, yp - ym, xp + xm, yp + ym

    source_z = sources[shot, 0] - d * depth_len
    source_x = sources[shot, 1]
    source_y = sources[shot, 2]
    mute_xy = (jnp.abs(row - source_x) <= MUTE) & (jnp.abs(lane - source_y) <= MUTE)

    current, previous = field_a, field_b
    for i in range(steps):
        extra = reach - i
        final = i == steps - 1

        def layer(f, before, here, after, owned, i=i, final=final, cur=current, prev=previous):
            v, dx, dy, sx, sy = here
            twice = 2.0 * v
            slopes = (
                after[0] - twice + before[0],
                sx - twice,
                sy - twice,
                after[1] - before[1],
                after[2] - before[2],
                under(dy) - over(dy),
            )
            acc = coef[0, f + reach] * slopes[0]
            for c in range(1, 6):
                acc = acc + coef[c, f + reach] * slopes[c]
            new = twice - prev[f + halo] + acc + inj[i, f + reach]
            if final:
                adjoint_first[0, f] = new
            else:
                prev[f + halo] = new
            if owned:
                wave = forward[i, 0, f].astype(F32)
                cross_wave = wave * 0.25
                for c in range(6):
                    term = (wave if c < 3 else cross_wave) * slopes[c]
                    if i:
                        term = totals[c, f] + term
                    if final:
                        hidden = mute_xy & (jnp.abs(f - source_z) <= MUTE)
                        term = jnp.where(hidden, 0.0, term)
                    totals[c, f] = term

        def run(first, stop, owned, carry, cur=current, layer=layer):
            def body(f, carry):
                before, here = carry
                after = sides(cur[f + 1 + halo])
                layer(f, before, here, after, owned)
                return here[:3], after
            return lax.fori_loop(first, stop, body, carry)

        carry = (sides(current[halo - extra - 1])[:3], sides(current[halo - extra]))
        if extra:
            carry = run(-extra, 0, False, carry)
        carry = run(0, depth_len, True, carry)
        if extra:
            carry = run(depth_len, depth_len + extra, False, carry)
        current, previous = previous, current

    push_field = pltpu.make_async_copy(adjoint_first, adjoint_hbm, out_sem.at[0])
    push_field.start()

    fine_16 = lax.broadcasted_iota(jnp.int32, (coarse_rows, cols), 0)
    last_depth = jnp.where(has_down, 0.0, 0.5)
    for c in range(6):
        lanes = slice((c // 3) * cols, (c // 3) * cols + cols)
        for l in range(coarse_len + 1):
            if l == coarse_len:
                value = 0.5 * totals[c, depth_len - 1]
            else:
                value = totals[c, 2 * l] + 0.5 * totals[c, 2 * l + 1]
                if l:
                    value = value + 0.5 * totals[c, 2 * l - 1]
                if l == coarse_len - 1:
                    value = value + last_depth * totals[c, depth_len - 1]
            restr[c, l] = value
            even = restr[c, l, pl.ds(0, coarse_rows, stride=2), :]
            odd = restr[c, l, pl.ds(1, coarse_rows, stride=2), :]
            earlier = jnp.where(fine_16 == 0, 0.0, pltpu.roll(odd, 1, 0))
            tail = jnp.where(fine_16 == coarse_rows - 1, odd, 0.0)
            value = even + 0.5 * (odd + earlier + tail)
            for s in range(shots):
                piece = value[s * rl:(s + 1) * rl]
                if l == coarse_len:
                    lhs_rim[s, (c % 3) * rl:(c % 3 + 1) * rl, lanes] = piece
                else:
                    first = (l * 3 + c % 3) * rl
                    lhs_main[s, first:first + rl, lanes] = piece

    main_rows, rim_rows = lhs_main.shape[1], lhs_rim.shape[1]
    outcome = split_dot(
        coarsen_ref[...], lhs_main[...].reshape(shots * main_rows, 2 * cols), "values_left")
    send_main[...] = outcome.reshape(shots, main_rows, 2 * half_cols)
    outcome = split_dot(
        coarsen_ref[...], lhs_rim[...].reshape(shots * rim_rows, 2 * cols), "values_left")
    send_rim[...] = outcome.reshape(shots, rim_rows, 2 * half_cols)

    def main_copy(t, sending):
        peer = other(t)
        slot = me if sending else peer
        return pltpu.make_async_remote_copy(
            src_ref=send_main.at[peer], dst_ref=recv_main.at[slot],
            send_sem=ms_sem.at[t], recv_sem=mr_sem.at[slot],
            device_id={"shot": peer}, device_id_type=MESH)

    def rim_copy(o, sending):
        peer = lax.rem(me + o, shots) if sending else lax.rem(me + shots - o, shots)
        slot = me if sending else peer
        return pltpu.make_async_remote_copy(
            src_ref=send_rim.at[peer], dst_ref=recv_rim.at[slot],
            send_sem=rs_sem.at[o], recv_sem=rr_sem.at[slot],
            device_id={"depth": d + 1 if sending else d - 1, "shot": peer}, device_id_type=MESH)

    for t in range(shots - 1):
        main_copy(t, True).start()

    @pl.when(has_down)
    def _():
        for o in range(shots):
            rim_copy(o, True).start()

    result = send_main[me]
    for t in range(shots - 1):
        main_copy(t, False).wait_recv()
        result = result + recv_main[other(t)]
    total[0] = result

    @pl.when(has_up)
    def _():
        rim_sum = None
        for o in range(shots):
            rim_copy(o, False).wait_recv()
            piece = recv_rim[lax.rem(me + shots - o, shots)]
            rim_sum = piece if rim_sum is None else rim_sum + piece
        total[0, 0:3 * rl] = total[0, 0:3 * rl] + rim_sum[0:3 * rl]

    result = total[0] * (1.0 / steps)
    total[0] = result
    total[1] = pltpu.roll(result, half_cols, 1)
    for l in range(coarse_len):
        for c in range(3):
            first = (l * 3 + c) * rl
            gradients[c, l] = total[0, first:first + rl, 0:half_cols]
            gradients[c + 3, l] = total[1, first:first + rl, 0:half_cols]

    push_gradients = pltpu.make_async_copy(gradients, gradients_hbm, out_sem.at[1])
    push_gradients.start()

    for t in range(shots - 1):
        gather_copy(t, True).wait_send()
        main_copy(t, True).wait_send()

    @pl.when(has_down)
    def _():
        for args in both:
            field_down(*args, True).wait_send()
        for slot in range(shots):
            model_down(slot, True).wait_send()
        for o in range(shots):
            rim_copy(o, True).wait_send()

    @pl.when(has_up)
    def _():
        for args in both:
            field_up(*args, True).wait_send()
        for slot in range(shots):
            model_up(slot, True).wait_send()

    push_field.wait()
    push_gradients.wait()


def up8(n):
    return (n + 7) // 8 * 8


def on_device(
    forward, adjoint_last, adjoint_late, residuals, source_cells, receiver_cells, assignment, model
):
    steps, shots_here, depth_len, rows, cols = forward.shape
    channels, coarse_len, rl, half_cols = model.shape
    shots = lax.axis_size("shot")
    assert shots_here == 1 and coarse_len == 4 and steps == 4 and channels == 6
    window = depth_len + 2 * steps - 2
    coarse_rows = shots * rl
    field = (depth_len + 2 * steps, rows, cols)
    main_rows, rim_rows = up8(coarse_len * 3 * rl), up8(3 * rl)
    dma = pltpu.SemaphoreType.DMA
    hbm = pl.BlockSpec(memory_space=pltpu.HBM)
    anywhere = pl.BlockSpec(memory_space=pl.ANY)
    receivers = jnp.transpose(receiver_cells, (2, 0, 1))
    smem = pl.BlockSpec(memory_space=pltpu.SMEM)
    return pl.pallas_call(
        kernel,
        name="adjoint_gradient",
        out_shape=(
            jax.ShapeDtypeStruct(adjoint_last.shape, F32),
            jax.ShapeDtypeStruct(model.shape, F32),
        ),
        in_specs=[hbm] * 6 + [smem] * 2,
        out_specs=(anywhere, anywhere),
        scratch_shapes=[
            pltpu.VMEM(forward.shape, forward.dtype),
            pltpu.VMEM(adjoint_last.shape, F32),
            pltpu.VMEM(adjoint_late.shape, F32),
            pltpu.VMEM(residuals.shape, F32),
            pltpu.VMEM(receivers.shape, receivers.dtype),
            pltpu.VMEM(model.shape, F32),
            pltpu.VMEM(adjoint_last.shape, F32),
            pltpu.VMEM(model.shape, F32),
            pltpu.VMEM((shots, 4, 6 * rl, 2 * half_cols), F32),
            pltpu.VMEM((6, 8, coarse_rows, cols), F32),
            pltpu.VMEM((6, 8, rows, cols), F32),
            pltpu.VMEM((6, window, rows, cols), F32),
            pltpu.VMEM(field, F32),
            pltpu.VMEM(field, F32),
            pltpu.VMEM((steps, window, rows, cols), F32),
            pltpu.VMEM((6, depth_len, rows, cols), F32),
            pltpu.VMEM((6, coarse_len + 1, rows, cols), F32),
            pltpu.VMEM((shots, main_rows, 2 * cols), F32),
            pltpu.VMEM((shots, rim_rows, 2 * cols), F32),
            pltpu.VMEM((shots, main_rows, 2 * half_cols), F32),
            pltpu.VMEM((shots, rim_rows, 2 * half_cols), F32),
            pltpu.VMEM((shots, main_rows, 2 * half_cols), F32),
            pltpu.VMEM((shots, rim_rows, 2 * half_cols), F32),
            pltpu.VMEM((2, main_rows, 2 * half_cols), F32),
            pltpu.VMEM((2 * cols, 2 * half_cols), BF16),
            dma((shots,)), dma((shots,)),
            dma((2, 2)), dma((2, 2)),
            dma((2, shots)), dma((2, shots)),
            dma((shots,)), dma((shots,)),
            dma((shots,)), dma((shots,)),
            dma((6,)), dma((2,)),
        ],
        compiler_params=pltpu.CompilerParams(
            collective_id=0, has_side_effects=True),
    )(
        forward, adjoint_last, adjoint_late, residuals,
        receivers, model, assignment, source_cells,
    )


def solution(mesh):
    placed = (
        P(None, ("grp", "shot"), "depth", None, None),
        P(("grp", "shot"), "depth", None, None),
        P(("grp", "shot"), "depth", None, None),
        P(("grp", "shot"), None, None),
        P("grp", None),
        P("grp", None, None),
        P("grp"),
        P(None, ("grp", "depth"), "shot", None),
    )
    return jax.shard_map(
        on_device,
        mesh=mesh,
        in_specs=placed,
        out_specs=(
            P(("grp", "shot"), "depth", None, None),
            P(None, ("grp", "depth"), "shot", None),
        ),
        check_vma=False,
    )
```

```python
import functools

import jax
import jax.numpy as jnp
from jax import lax
from jax.experimental import pallas as pl
from jax.experimental.pallas import tpu as pltpu
from jax.sharding import PartitionSpec as P

MUTE = 3
TIME_SQUARED = 0.2
MESH = pl.DeviceIdType.MESH
F32 = jnp.float32
BF16 = jnp.bfloat16


def split_dot(exact, values, contract):
    high = values.astype(BF16)
    low = (values - high.astype(F32)).astype(BF16)
    return exact_dot(exact, high, contract) + exact_dot(exact, low, contract)


def exact_dot(exact, part, contract):
    if contract == "values_left":
        return lax.dot_general(part, exact, (((1,), (0,)), ((), ())), preferred_element_type=F32)
    return lax.dot_general(exact, part, (((1,), (1,)), ((), ())), preferred_element_type=F32)


def kernel(
    forward_hbm, last_hbm, late_hbm, residuals_hbm, receivers_hbm, model_hbm, assignment, sources,
    adjoint_hbm, gradients_hbm,
    forward, last, late, residuals, receivers, model, adjoint_first, gradients,
    gbuf, coarse_y, fine_x, coef, field_a, field_b, inj, totals, restr, lhs_main, lhs_rim,
    send_main, send_rim, recv_main, recv_rim, total, coarsen_ref,
    gs_sem, gr_sem, hs_sem, hr_sem, fs_sem, fr_sem, ms_sem, mr_sem, rs_sem, rr_sem, in_sem, out_sem,
):
    steps = forward.shape[0]
    depth_len, rows, cols = last.shape[1:]
    coarse_len, rl, half_cols = model.shape[1:]
    shots = lax.axis_size("shot")
    depths = lax.axis_size("depth")
    me = lax.axis_index("shot")
    d = lax.axis_index("depth")
    has_up = d > 0
    has_down = d < depths - 1
    halo = steps
    reach = steps - 1
    window = depth_len + 2 * reach
    coarse_rows = shots * rl

    barrier = pltpu.get_barrier_semaphore()

    def greet(device):
        pl.semaphore_signal(barrier, inc=1, device_id=device, device_id_type=MESH)

    for o in range(1, shots):
        greet({"shot": lax.rem(me + o, shots)})

    @pl.when(has_up)
    def _():
        greet({"depth": d - 1})

    @pl.when(has_down)
    def _():
        greet({"depth": d + 1})

    pulls = [
        pltpu.make_async_copy(source, dest, in_sem.at[k])
        for k, (source, dest) in enumerate((
            (model_hbm, model), (last_hbm, last), (late_hbm, late), (receivers_hbm, receivers),
            (residuals_hbm, residuals), (forward_hbm, forward)))
    ]
    for pull in pulls:
        pull.start()
    pulls[0].wait()

    for l in range(coarse_len):
        for c in range(3):
            pair = jnp.concatenate([model[c, l], model[c + 3, l]], axis=-1)
            first = ((l % 2) * 3 + c) * rl
            gbuf[me, 1 + l // 2, first:first + rl, :] = pair

    beside = jnp.where(has_up, 1, 0) + jnp.where(has_down, 1, 0)
    pl.semaphore_wait(barrier, shots - 1 + beside)

    later = shots - 1 - me

    def other(t):
        return jnp.where(t < later, shots - 1 - t, t - later)

    def gather_copy(t, sending):
        peer = other(t)
        slot = me if sending else peer
        return pltpu.make_async_remote_copy(
            src_ref=gbuf.at[slot, 1:3], dst_ref=gbuf.at[slot, 1:3],
            send_sem=gs_sem.at[t], recv_sem=gr_sem.at[slot],
            device_id={"shot": peer}, device_id_type=MESH)

    for t in range(shots - 1):
        gather_copy(t, True).start()

    def field_down(which, source, dest, width, sending):
        return pltpu.make_async_remote_copy(
            src_ref=source.at[0, depth_len - width:depth_len],
            dst_ref=dest.at[halo - width:halo],
            send_sem=hs_sem.at[0, which], recv_sem=hr_sem.at[0, which],
            device_id={"depth": d + 1 if sending else d - 1}, device_id_type=MESH)

    def field_up(which, source, dest, width, sending):
        return pltpu.make_async_remote_copy(
            src_ref=source.at[0, 0:width],
            dst_ref=dest.at[halo + depth_len:halo + depth_len + width],
            send_sem=hs_sem.at[1, which], recv_sem=hr_sem.at[1, which],
            device_id={"depth": d - 1 if sending else d + 1}, device_id_type=MESH)

    both = ((0, last, field_a, halo), (1, late, field_b, reach))

    def model_down(slot, sending):
        return pltpu.make_async_remote_copy(
            src_ref=gbuf.at[slot, 2], dst_ref=gbuf.at[slot, 0],
            send_sem=fs_sem.at[0, slot], recv_sem=fr_sem.at[0, slot],
            device_id={"depth": d + 1 if sending else d - 1}, device_id_type=MESH)

    def model_up(slot, sending):
        return pltpu.make_async_remote_copy(
            src_ref=gbuf.at[slot, 1], dst_ref=gbuf.at[slot, 3],
            send_sem=fs_sem.at[1, slot], recv_sem=fr_sem.at[1, slot],
            device_id={"depth": d - 1 if sending else d + 1}, device_id_type=MESH)

    def spread(slot):
        @pl.when(has_down)
        def _():
            model_down(slot, True).start()

        @pl.when(has_up)
        def _():
            model_up(slot, True).start()

    spread(me)
    pulls[1].wait()
    pulls[2].wait()

    @pl.when(has_down)
    def _():
        for args in both:
            field_down(*args, True).start()

    @pl.when(has_up)
    def _():
        for args in both:
            field_up(*args, True).start()

    zeros_halo = jnp.zeros((halo, rows, cols), F32)

    @pl.when(jnp.logical_not(has_up))
    def _():
        field_a[0:halo] = zeros_halo
        field_b[0:halo] = zeros_halo

    @pl.when(jnp.logical_not(has_down))
    def _():
        field_a[halo + depth_len:] = zeros_halo
        field_b[halo + depth_len:] = zeros_halo

    field_a[halo:halo + depth_len] = last[0]
    field_b[halo:halo + depth_len] = late[0]

    pulls[3].wait()
    pulls[4].wait()
    shot = assignment[me]
    picked = []
    for k in range(3):
        chosen = jnp.zeros((1, receivers.shape[2]), jnp.int32)
        for j in range(receivers.shape[1]):
            chosen = chosen + jnp.where(shot == j, receivers[k, j:j + 1, :], 0)
        picked.append(chosen)
    place = (picked[0] - d * depth_len + reach) * rows + picked[1]
    count = receivers.shape[2]
    spot = lax.broadcasted_iota(jnp.int32, (window * rows, count), 0) == place
    spot = jnp.where(spot, 1.0, 0.0).astype(BF16)
    column = lax.broadcasted_iota(jnp.int32, (cols, count), 0) == picked[2]
    for i in range(steps):
        placed = jnp.where(column, residuals[0, i:i + 1, :], 0.0)
        high = placed.astype(BF16)
        low = (placed - high.astype(F32)).astype(BF16)
        both_parts = exact_dot(spot, jnp.concatenate([high, low], axis=0), "values_right")
        inj[i] = (both_parts[:, 0:cols] + both_parts[:, cols:]).reshape(window, rows, cols)

    c_in = lax.broadcasted_iota(jnp.int32, (2 * half_cols, 2 * cols), 0)
    f_out = lax.broadcasted_iota(jnp.int32, (2 * half_cols, 2 * cols), 1)
    same = (c_in >= half_cols) == (f_out >= cols)
    ci = jnp.where(c_in >= half_cols, c_in - half_cols, c_in)
    fo = jnp.where(f_out >= cols, f_out - cols, f_out)
    weight = jnp.where(fo == 2 * ci, 1.0, 0.0)
    weight = weight + jnp.where((fo == 2 * ci + 1) | (fo == 2 * ci - 1), 0.5, 0.0)
    weight = weight + jnp.where((fo == cols - 1) & (ci == half_cols - 1), 0.5, 0.0)
    refine_y = jnp.where(same, weight, 0.0).astype(BF16)

    f_in = lax.broadcasted_iota(jnp.int32, (2 * cols, 2 * half_cols), 0)
    c_out = lax.broadcasted_iota(jnp.int32, (2 * cols, 2 * half_cols), 1)
    same = (f_in >= cols) == (c_out >= half_cols)
    fi = jnp.where(f_in >= cols, f_in - cols, f_in)
    co = jnp.where(c_out >= half_cols, c_out - half_cols, c_out)
    weight = jnp.where(fi == 2 * co, 1.0, 0.0)
    weight = weight + jnp.where((fi == 2 * co + 1) | (fi == 2 * co - 1), 0.5, 0.0)
    weight = weight + jnp.where((fi == cols - 1) & (co == half_cols - 1), 0.5, 0.0)
    coarsen_y = jnp.where(same, weight, 0.0).astype(BF16)
    coarsen_ref[...] = coarsen_y

    pulls[5].wait()
    for t in range(shots - 1):
        gather_copy(t, False).wait_recv()
        spread(other(t))

    row16 = lax.broadcasted_iota(jnp.int32, (coarse_rows, cols), 0)

    def refine_group(group):
        width = 6 * rl
        merged = width % 8 == 0
        if merged:
            slab = gbuf[:, group].reshape(shots * width, 2 * half_cols)
            slab = split_dot(refine_y, slab, "values_left") * TIME_SQUARED
        for s in range(shots):
            if merged:
                refined = slab[s * width:(s + 1) * width]
            else:
                refined = split_dot(refine_y, gbuf[s, group], "values_left") * TIME_SQUARED
            for l2 in range(2):
                for c in range(3):
                    first = (l2 * 3 + c) * rl
                    piece = refined[first:first + rl]
                    coarse_y[c, 2 * group + l2, s * rl:(s + 1) * rl, :] = piece[:, 0:cols]
                    coarse_y[c + 3, 2 * group + l2, s * rl:(s + 1) * rl, :] = piece[:, cols:]
        for c in range(6):
            scale = 1.0 if c < 3 else 0.25
            for l in (2 * group, 2 * group + 1):
                here = coarse_y[c, l] * scale
                after = pltpu.roll(here, coarse_rows - 1, 0)
                after = jnp.where(row16 == coarse_rows - 1, here, after)
                fine_x[c, l, pl.ds(0, coarse_rows, stride=2), :] = here
                fine_x[c, l, pl.ds(1, coarse_rows, stride=2), :] = (here + after) * 0.5

    def refine_depth(first, stop):
        for c in range(6):
            for f in range(first, stop):
                k = f // 2 + 2
                value = fine_x[c, k]
                if f % 2:
                    after = fine_x[c, k + 1]
                    if f == depth_len - 1:
                        after = jnp.where(has_down, after, value)
                    value = (value + after) * 0.5
                if f < 0:
                    value = jnp.where(has_up, value, 0.0)
                if f >= depth_len:
                    value = jnp.where(has_down, value, 0.0)
                coef[c, f + reach] = value

    refine_group(1)
    refine_group(2)
    refine_depth(0, depth_len - 1)

    @pl.when(has_up)
    def _():
        for slot in range(shots):
            model_down(slot, False).wait_recv()

    @pl.when(has_down)
    def _():
        for slot in range(shots):
            model_up(slot, False).wait_recv()

    refine_group(0)
    refine_group(3)
    refine_depth(-reach, 0)
    refine_depth(depth_len - 1, depth_len + reach)

    @pl.when(has_up)
    def _():
        for args in both:
            field_down(*args, False).wait_recv()

    @pl.when(has_down)
    def _():
        for args in both:
            field_up(*args, False).wait_recv()

    lane = lax.broadcasted_iota(jnp.int32, (rows, cols), 1)
    row = lax.broadcasted_iota(jnp.int32, (rows, cols), 0)
    lane_first, lane_last = lane == 0, lane == cols - 1
    row_first, row_last = row == 0, row == rows - 1

    def right(v):
        return jnp.where(lane_last, 0.0, pltpu.roll(v, cols - 1, 1))

    def left(v):
        return jnp.where(lane_first, 0.0, pltpu.roll(v, 1, 1))

    def under(v):
        return jnp.where(row_last, 0.0, pltpu.roll(v, rows - 1, 0))

    def over(v):
        return jnp.where(row_first, 0.0, pltpu.roll(v, 1, 0))

    def sides(v):
        xp, xm, yp, ym = under(v), over(v), right(v), left(v)
        return v, xp - xm, yp - ym, xp + xm, yp + ym

    source_z = sources[shot, 0] - d * depth_len
    source_x = sources[shot, 1]
    source_y = sources[shot, 2]
    mute_xy = (jnp.abs(row - source_x) <= MUTE) & (jnp.abs(lane - source_y) <= MUTE)

    current, previous = field_a, field_b
    for i in range(steps):
        extra = reach - i
        final = i == steps - 1

        def layer(f, before, here, after, owned, i=i, final=final, cur=current, prev=previous):
            v, dx, dy, sx, sy = here
            twice = 2.0 * v
            slopes = (
                after[0] - twice + before[0],
                sx - twice,
                sy - twice,
                after[1] - before[1],
                after[2] - before[2],
                under(dy) - over(dy),
            )
            acc = coef[0, f + reach] * slopes[0]
            for c in range(1, 6):
                acc = acc + coef[c, f + reach] * slopes[c]
            new = twice - prev[f + halo] + acc + inj[i, f + reach]
            if final:
                adjoint_first[0, f] = new
            else:
                prev[f + halo] = new
            if owned:
                wave = forward[i, 0, f].astype(F32)
                cross_wave = wave * 0.25
                for c in range(6):
                    term = (wave if c < 3 else cross_wave) * slopes[c]
                    if i:
                        term = totals[c, f] + term
                    if final:
                        hidden = mute_xy & (jnp.abs(f - source_z) <= MUTE)
                        term = jnp.where(hidden, 0.0, term)
                    totals[c, f] = term

        def run(first, stop, owned, carry, cur=current, layer=layer):
            before, here = carry
            for f in range(first, stop):
                after = sides(cur[f + 1 + halo])
                layer(f, before, here, after, owned)
                before, here = here[:3], after
            return before, here

        carry = (sides(current[halo - extra - 1])[:3], sides(current[halo - extra]))
        if extra:
            carry = run(-extra, 0, False, carry)
        carry = run(0, depth_len, True, carry)
        if extra:
            carry = run(depth_len, depth_len + extra, False, carry)
        current, previous = previous, current

    push_field = pltpu.make_async_copy(adjoint_first, adjoint_hbm, out_sem.at[0])
    push_field.start()

    fine_16 = lax.broadcasted_iota(jnp.int32, (coarse_rows, cols), 0)
    last_depth = jnp.where(has_down, 0.0, 0.5)
    for c in range(6):
        lanes = slice((c // 3) * cols, (c // 3) * cols + cols)
        for l in range(coarse_len + 1):
            if l == coarse_len:
                value = 0.5 * totals[c, depth_len - 1]
            else:
                value = totals[c, 2 * l] + 0.5 * totals[c, 2 * l + 1]
                if l:
                    value = value + 0.5 * totals[c, 2 * l - 1]
                if l == coarse_len - 1:
                    value = value + last_depth * totals[c, depth_len - 1]
            restr[c, l] = value
            even = restr[c, l, pl.ds(0, coarse_rows, stride=2), :]
            odd = restr[c, l, pl.ds(1, coarse_rows, stride=2), :]
            earlier = jnp.where(fine_16 == 0, 0.0, pltpu.roll(odd, 1, 0))
            tail = jnp.where(fine_16 == coarse_rows - 1, odd, 0.0)
            value = even + 0.5 * (odd + earlier + tail)
            for s in range(shots):
                piece = value[s * rl:(s + 1) * rl]
                if l == coarse_len:
                    lhs_rim[s, (c % 3) * rl:(c % 3 + 1) * rl, lanes] = piece
                else:
                    first = (l * 3 + c % 3) * rl
                    lhs_main[s, first:first + rl, lanes] = piece

    main_rows, rim_rows = lhs_main.shape[1], lhs_rim.shape[1]
    outcome = split_dot(
        coarsen_ref[...], lhs_main[...].reshape(shots * main_rows, 2 * cols), "values_left")
    send_main[...] = outcome.reshape(shots, main_rows, 2 * half_cols)
    outcome = split_dot(
        coarsen_ref[...], lhs_rim[...].reshape(shots * rim_rows, 2 * cols), "values_left")
    send_rim[...] = outcome.reshape(shots, rim_rows, 2 * half_cols)

    def main_copy(t, sending):
        peer = other(t)
        slot = me if sending else peer
        return pltpu.make_async_remote_copy(
            src_ref=send_main.at[peer], dst_ref=recv_main.at[slot],
            send_sem=ms_sem.at[t], recv_sem=mr_sem.at[slot],
            device_id={"shot": peer}, device_id_type=MESH)

    def rim_copy(o, sending):
        peer = lax.rem(me + o, shots) if sending else lax.rem(me + shots - o, shots)
        slot = me if sending else peer
        return pltpu.make_async_remote_copy(
            src_ref=send_rim.at[peer], dst_ref=recv_rim.at[slot],
            send_sem=rs_sem.at[o], recv_sem=rr_sem.at[slot],
            device_id={"depth": d + 1 if sending else d - 1, "shot": peer}, device_id_type=MESH)

    for t in range(shots - 1):
        main_copy(t, True).start()

    @pl.when(has_down)
    def _():
        for o in range(shots):
            rim_copy(o, True).start()

    result = send_main[me]
    for t in range(shots - 1):
        main_copy(t, False).wait_recv()
        result = result + recv_main[other(t)]
    total[0] = result

    @pl.when(has_up)
    def _():
        rim_sum = None
        for o in range(shots):
            rim_copy(o, False).wait_recv()
            piece = recv_rim[lax.rem(me + shots - o, shots)]
            rim_sum = piece if rim_sum is None else rim_sum + piece
        total[0, 0:3 * rl] = total[0, 0:3 * rl] + rim_sum[0:3 * rl]

    result = total[0] * (1.0 / steps)
    total[0] = result
    total[1] = pltpu.roll(result, half_cols, 1)
    for l in range(coarse_len):
        for c in range(3):
            first = (l * 3 + c) * rl
            gradients[c, l] = total[0, first:first + rl, 0:half_cols]
            gradients[c + 3, l] = total[1, first:first + rl, 0:half_cols]

    push_gradients = pltpu.make_async_copy(gradients, gradients_hbm, out_sem.at[1])
    push_gradients.start()

    for t in range(shots - 1):
        gather_copy(t, True).wait_send()
        main_copy(t, True).wait_send()

    @pl.when(has_down)
    def _():
        for args in both:
            field_down(*args, True).wait_send()
        for slot in range(shots):
            model_down(slot, True).wait_send()
        for o in range(shots):
            rim_copy(o, True).wait_send()

    @pl.when(has_up)
    def _():
        for args in both:
            field_up(*args, True).wait_send()
        for slot in range(shots):
            model_up(slot, True).wait_send()

    push_field.wait()
    push_gradients.wait()


def up8(n):
    return (n + 7) // 8 * 8


def on_device(
    forward, adjoint_last, adjoint_late, residuals, source_cells, receiver_cells, assignment, model
):
    steps, shots_here, depth_len, rows, cols = forward.shape
    channels, coarse_len, rl, half_cols = model.shape
    shots = lax.axis_size("shot")
    assert shots_here == 1 and coarse_len == 4 and steps == 4 and channels == 6
    window = depth_len + 2 * steps - 2
    coarse_rows = shots * rl
    field = (depth_len + 2 * steps, rows, cols)
    main_rows, rim_rows = up8(coarse_len * 3 * rl), up8(3 * rl)
    dma = pltpu.SemaphoreType.DMA
    hbm = pl.BlockSpec(memory_space=pltpu.HBM)
    anywhere = pl.BlockSpec(memory_space=pl.ANY)
    receivers = jnp.transpose(receiver_cells, (2, 0, 1))
    smem = pl.BlockSpec(memory_space=pltpu.SMEM)
    return pl.pallas_call(
        kernel,
        name="adjoint_gradient",
        out_shape=(
            jax.ShapeDtypeStruct(adjoint_last.shape, F32),
            jax.ShapeDtypeStruct(model.shape, F32),
        ),
        in_specs=[hbm] * 6 + [smem] * 2,
        out_specs=(anywhere, anywhere),
        scratch_shapes=[
            pltpu.VMEM(forward.shape, forward.dtype),
            pltpu.VMEM(adjoint_last.shape, F32),
            pltpu.VMEM(adjoint_late.shape, F32),
            pltpu.VMEM(residuals.shape, F32),
            pltpu.VMEM(receivers.shape, receivers.dtype),
            pltpu.VMEM(model.shape, F32),
            pltpu.VMEM(adjoint_last.shape, F32),
            pltpu.VMEM(model.shape, F32),
            pltpu.VMEM((shots, 4, 6 * rl, 2 * half_cols), F32),
            pltpu.VMEM((6, 8, coarse_rows, cols), F32),
            pltpu.VMEM((6, 8, rows, cols), F32),
            pltpu.VMEM((6, window, rows, cols), F32),
            pltpu.VMEM(field, F32),
            pltpu.VMEM(field, F32),
            pltpu.VMEM((steps, window, rows, cols), F32),
            pltpu.VMEM((6, depth_len, rows, cols), F32),
            pltpu.VMEM((6, coarse_len + 1, rows, cols), F32),
            pltpu.VMEM((shots, main_rows, 2 * cols), F32),
            pltpu.VMEM((shots, rim_rows, 2 * cols), F32),
            pltpu.VMEM((shots, main_rows, 2 * half_cols), F32),
            pltpu.VMEM((shots, rim_rows, 2 * half_cols), F32),
            pltpu.VMEM((shots, main_rows, 2 * half_cols), F32),
            pltpu.VMEM((shots, rim_rows, 2 * half_cols), F32),
            pltpu.VMEM((2, main_rows, 2 * half_cols), F32),
            pltpu.VMEM((2 * cols, 2 * half_cols), BF16),
            dma((shots,)), dma((shots,)),
            dma((2, 2)), dma((2, 2)),
            dma((2, shots)), dma((2, shots)),
            dma((shots,)), dma((shots,)),
            dma((shots,)), dma((shots,)),
            dma((6,)), dma((2,)),
        ],
        compiler_params=pltpu.CompilerParams(
            collective_id=0, has_side_effects=True),
    )(
        forward, adjoint_last, adjoint_late, residuals,
        receivers, model, assignment, source_cells,
    )


def solution(mesh):
    placed = (
        P(None, ("grp", "shot"), "depth", None, None),
        P(("grp", "shot"), "depth", None, None),
        P(("grp", "shot"), "depth", None, None),
        P(("grp", "shot"), None, None),
        P("grp", None),
        P("grp", None, None),
        P("grp"),
        P(None, ("grp", "depth"), "shot", None),
    )
    return jax.shard_map(
        on_device,
        mesh=mesh,
        in_specs=placed,
        out_specs=(
            P(("grp", "shot"), "depth", None, None),
            P(None, ("grp", "depth"), "shot", None),
        ),
        check_vma=False,
    )
```
